32 devices in a mesh: dp: 8 (over y, x, core), tp: 4 (over z).
Axes of the slice: x: 2, y: 2, z: 4, core: 2. Of those that a mesh axis runs over, the one named last changes fastest.
Arguments:
- slope_up: float32 [8, 1280, 5120], P('dp', None, 'tp'), may hold values from -0.875 to 0.875
- slope_down: float32 [8, 5120, 1280], P('dp', 'tp'), may hold values from -0.875 to 0.875
- slope_norm: float32 [8, 1280], P('dp'), may hold values from -8 to 8
- slope_bias: float32 [8, 1280], P('dp'), may hold values from -8 to 8
- param_up: float32 [1280, 5120], P('dp', 'tp'), may hold values from -0.15625 to 0.15625
- param_down: float32 [5120, 1280], P('tp', 'dp'), may hold values from -0.078125 to 0.078125
- param_norm: float32 [1280], P('dp'), may hold values from 0.25 to 1.75
- param_bias: float32 [1280], P('dp'), may hold values from -3 to 3
- state_up: float32 [1280, 5120], P('dp', 'tp'), may hold values from -1.75 to 1.75
- state_down: float32 [5120, 1280], P('tp', 'dp'), may hold values from -1.75 to 1.75
- state_norm: float32 [1280], P('dp'), may hold values from -1.75 to 1.75
- state_bias: float32 [1280], P('dp'), may hold values from -1.75 to 1.75
Outputs:
- half_up: bfloat16 [1280, 5120], P(None, 'tp')
- half_down: bfloat16 [5120, 1280], P('tp')
- half_norm: bfloat16 [1280], replicated
- half_bias: bfloat16 [1280], replicated
- next_up: float32 [1280, 5120], P('dp', 'tp')
- next_down: float32 [5120, 1280], P('tp', 'dp')
- next_norm: float32 [1280], P('dp')
- next_bias: float32 [1280], P('dp')
- state_new_up: float32 [1280, 5120], P('dp', 'tp')
- state_new_down: float32 [5120, 1280], P('tp', 'dp')
- state_new_norm: float32 [1280], P('dp')
- state_new_bias: float32 [1280], P('dp')
The draws below stay inside these ranges and needn't reach their ends.
All inputs are finite; a program needn't handle non-finite values.
Results may differ from the reference program's by a relative error of at most 0.009.
Values may be sent and summed in bfloat16 or wider, within the bound.
A program may use at most 64 MiB of HBM per device.

```python
import jax
import jax.numpy as jnp

WIDTH = 1280
INNER = 5120
REPLICAS = 8


def strengthened(values, rng, source, target, parts, factor):
    owner, partner = [(jnp.arange(values.shape[position]) // (values.shape[position] // parts)).reshape([-1 if axis == position else 1 for axis in range(values.ndim)]) for position in (source, target)]
    chosen = jax.random.permutation(rng, parts)[partner]
    strong = (owner == chosen) | (owner == (partner + parts // 2) % parts)
    return jnp.where(strong, factor * values, values)


def shard_levels(stream_key, shape, cuts, low, high):
    def one(dim, parts):
        heights = jax.random.uniform(jax.random.fold_in(jax.random.fold_in(stream_key, 6), dim), (parts,), jnp.float32, low / len(cuts), high / len(cuts))
        return jnp.repeat(jnp.exp(heights), shape[dim] // parts).reshape((-1,) + (1,) * (len(shape) - dim - 1))

    factor_of = one(*cuts[0])
    for cut in cuts[1:]:
        factor_of = factor_of * one(*cut)
    return factor_of


def normal_values(key, shape, deviation, bound, pieces=(), dtype=jnp.bfloat16):
    factor_of = shard_levels(key, shape, pieces, -0.22, 0.18) if pieces else 1.0
    array = jax.random.normal(key, shape, jnp.float32) * deviation * factor_of
    return jnp.minimum(jnp.maximum(array, -bound), bound).astype(dtype)


def bell_draw_with(stream_key, extent, spread, reach, split, heavy, kind=jnp.bfloat16):
    result = spread * jax.random.normal(stream_key, extent, jnp.float32)
    if split:
        result = result * shard_levels(stream_key, extent, split, -0.22, 0.18)
    return jnp.clip(strengthened(result, jax.random.fold_in(stream_key, 3), *heavy), -reach, reach).astype(kind)


def setup_inputs(seed: int = 0) -> dict:
    keys = jax.random.split(jax.random.key(seed), 13)
    slope_up = bell_draw_with(keys[0], (REPLICAS, WIDTH, INNER), 0.1, 0.875, ((0, 8), (2, 4)), (0, 1, 8, 2.0), jnp.float32)
    slope_down = bell_draw_with(keys[1], (REPLICAS, INNER, WIDTH), 0.1, 0.875, ((0, 8), (1, 4)), (0, 2, 8, 2.0), jnp.float32)
    slope_norm = bell_draw_with(keys[2], (REPLICAS, WIDTH), 1.0, 8.0, ((0, 8),), (0, 1, 8, 2.0), jnp.float32)
    slope_bias = bell_draw_with(keys[3], (REPLICAS, WIDTH), 1.0, 8.0, ((0, 8),), (0, 1, 8, 2.0), jnp.float32)
    param_up = normal_values(keys[4], (WIDTH, INNER), WIDTH ** -0.5, 0.15625, ((0, 8), (1, 4)), jnp.float32)
    param_down = normal_values(keys[5], (INNER, WIDTH), INNER ** -0.5, 0.078125, ((0, 4), (1, 8)), jnp.float32)
    param_norm = jnp.clip(1.0 + 0.15 * jax.random.normal(keys[6], (WIDTH,), jnp.float32), 0.25, 1.75)
    param_bias = normal_values(keys[7], (WIDTH,), 0.5, 3.0, ((0, 8),), jnp.float32)
    state_up = normal_values(keys[8], (WIDTH, INNER), 0.3, 1.75, ((0, 8), (1, 4)), jnp.float32)
    state_down = normal_values(keys[9], (INNER, WIDTH), 0.3, 1.75, ((0, 4), (1, 8)), jnp.float32)
    state_norm = normal_values(keys[10], (WIDTH,), 0.3, 1.75, ((0, 8),), jnp.float32)
    state_bias = normal_values(keys[11], (WIDTH,), 0.3, 1.75, ((0, 8),), jnp.float32)
    return dict(slope_up=slope_up, slope_down=slope_down, slope_norm=slope_norm, slope_bias=slope_bias, param_up=param_up, param_down=param_down, param_norm=param_norm, param_bias=param_bias, state_up=state_up, state_down=state_down, state_norm=state_norm, state_bias=state_bias)


learn_rate = 0.1
hold_rate = 0.7


def reference(slope_up, slope_down, slope_norm, slope_bias, param_up, param_down, param_norm, param_bias, state_up, state_down, state_norm, state_bias):
    mean_up = jnp.sum(slope_up.astype(jnp.float32), axis=0) * REPLICAS ** -0.5
    mean_down = jnp.sum(slope_down.astype(jnp.float32), axis=0) * REPLICAS ** -0.5
    mean_norm = jnp.sum(slope_norm.astype(jnp.float32), axis=0) * REPLICAS ** -0.5
    mean_bias = jnp.sum(slope_bias.astype(jnp.float32), axis=0) * REPLICAS ** -0.5
    state_new_up = hold_rate * state_up + mean_up
    next_up = param_up - learn_rate * state_new_up
    state_new_down = hold_rate * state_down + mean_down
    next_down = param_down - learn_rate * state_new_down
    state_new_norm = hold_rate * state_norm + mean_norm
    next_norm = param_norm - learn_rate * state_new_norm
    state_new_bias = hold_rate * state_bias + mean_bias
    next_bias = param_bias - learn_rate * state_new_bias
    half_up = next_up.astype(jnp.bfloat16)
    half_down = next_down.astype(jnp.bfloat16)
    half_norm = next_norm.astype(jnp.bfloat16)
    half_bias = next_bias.astype(jnp.bfloat16)
    return half_up, half_down, half_norm, half_bias, next_up, next_down, next_norm, next_bias, state_new_up, state_new_down, state_new_norm, state_new_bias
```

```python
import functools

import jax
import jax.numpy as jnp
from jax import lax
from jax.experimental import pallas as pl
from jax.experimental.pallas import tpu as pltpu
from jax.sharding import PartitionSpec as P

learn_rate = 0.1
hold_rate = 0.7
LANES = 128
AHEAD = 2
F32 = jnp.float32
BF16 = jnp.bfloat16
D2D, RS1, RS2, AG1, AG2, SH1, SH2 = range(7)


def slab_plan(columns):
    half = columns // LANES // 2
    widths = [half // 2, half - half // 2] if half > 1 else [half]
    plan, start = [], 0
    for width in widths:
        for axis in (0, 1):
            plan.append((start, width * LANES, axis))
            start += width * LANES
    return plan


def row_loop(rows, step, fn):
    def go(i, carry):
        fn(pl.ds(pl.multiple_of(i * step, step), step))
        return carry

    lax.fori_loop(0, rows // step, go, 0)


def kernel(
    replicas, plan,
    su, sd, sn, sb, pu, pd, pn, pb, tu, td, tn, tb,
    gu, hd, par, sta, vown, vhalf,
    fu, fd, bu, bd, r0, r1, r2, gd, vsend, vrecv, vin, vshard,
    send_sem, recv_sem, vsend_sem, vrecv_sem, load_sem, par_sem, vload_sem,
):
    chunk, columns = pu.shape
    width = replicas * chunk
    me = lax.axis_index("dp")
    c = lax.rem(me, 2)
    x = lax.rem(me // 2, 2)
    y = me // 4
    mate = me + 1 - 2 * c
    nbr = (me + 2 - 4 * x, me + 4 - 8 * y)
    rate = replicas ** (-0.5)
    slabs = [(m,) + s for m in (0, 1) for s in plan]
    per = len(plan)
    count = len(slabs)
    step = 32 if chunk % 32 == 0 else 16
    b, g = (bu, bd), (gu, gd)

    loads = []
    for i, (m, lo, w, _) in enumerate(slabs):
        if m == 0:
            cp = pltpu.make_async_copy(su.at[0, :, pl.ds(lo, w)], fu.at[:, pl.ds(lo, w)], load_sem.at[i])
        else:
            cp = pltpu.make_async_copy(sd.at[0, pl.ds(lo, w)], fd.at[pl.ds(lo, w)], load_sem.at[i])
        loads.append(cp)
    vloads = []
    for i, src in enumerate((sn, sb, pn, pb, tn, tb)):
        dst = vin.at[i] if i < 2 else vshard.at[i - 2]
        cp = pltpu.make_async_copy(src, dst, vload_sem.at[i])
        cp.start()
        vloads.append(cp)
    for cp in loads[:AHEAD]:
        cp.start()
    ploads = []
    for i, (src, dst) in enumerate(((pu, par.at[0]), (pd, par.at[1]), (tu, sta.at[0]), (td, sta.at[1]))):
        ploads.append(pltpu.make_async_copy(src, dst, par_sem.at[i]))

    barrier = pltpu.get_barrier_semaphore()
    for i in range(1, replicas):
        pl.semaphore_signal(
            barrier, inc=1, device_id={"dp": lax.rem(me + i, replicas)}, device_id_type=pl.DeviceIdType.MESH
        )

    vw = columns_pad(chunk)
    vsend[...] = jnp.zeros_like(vsend)
    for cp in vloads:
        cp.wait()
    for row in (0, 1):
        vsend[row : row + 1, 0:width] = vin[row]
        vsend[row : row + 1, width : width + chunk] = vshard[row]
        vsend[row : row + 1, width + vw : width + vw + chunk] = vshard[2 + row]
    vrecv[me] = vsend[...]

    def convert(i):
        m, lo, w, _ = slabs[i]
        loads[i].wait()
        for cp in loads[i + AHEAD : i + AHEAD + 1] if i + AHEAD < count else ploads if i + AHEAD == count else ():
            cp.start()
        if m == 0:
            for k in range(replicas):
                dst = bu.at[k // 4, (k // 2) % 2, k % 2]

                def go(rows, k=k, dst=dst):
                    src = pl.ds(pl.multiple_of(k * chunk + rows.start, step), step)
                    dst[rows, lo : lo + w] = fu[src, lo : lo + w].astype(BF16)

                row_loop(chunk, step, go)
        else:
            for block in range(width // LANES):
                first = block * LANES
                turned = fd[lo : lo + w, first : first + LANES].T.astype(BF16)
                done = 0
                while done < LANES:
                    k, off = divmod(first + done, chunk)
                    n = min(LANES - done, chunk - off)
                    bd[k // 4, (k // 2) % 2, k % 2, off : off + n, lo : lo + w] = turned[done : done + n]
                    done += n

    def copy(i, kind, src, dst, target):
        cp = pltpu.make_async_remote_copy(
            src_ref=src, dst_ref=dst,
            send_sem=send_sem.at[kind, i], recv_sem=recv_sem.at[kind, i],
            device_id={"dp": target}, device_id_type=pl.DeviceIdType.MESH,
        )
        cp.start()
        return cp

    copies = {}

    def swap(i):
        m, lo, w, _ = slabs[i]
        cols = pl.ds(lo, w)
        copies[i, D2D] = copy(i, D2D, b[m].at[:, :, 1 - c, :, cols], r0.at[m, :, :, :, cols], mate)

    def add_to(dst, src, lo, w):
        def go(rows):
            cols = slice(lo, lo + w)
            dst[rows, cols] = (dst[rows, cols].astype(F32) + src[rows, cols].astype(F32)).astype(BF16)

        row_loop(chunk, step, go)

    def rs1(i):
        m, lo, w, axis = slabs[i]
        cols = pl.ds(lo, w)
        copies[i, D2D].wait_recv()
        for far in (1, 0):
            for j in (0, 1):
                if axis == 0:
                    yy, xx = j, (1 - x if far else x)
                else:
                    yy, xx = (1 - y if far else y), j
                add_to(b[m].at[yy, xx, c], r0.at[m, yy, xx], lo, w)
            if far:
                src = b[m].at[:, 1 - x, c, :, cols] if axis == 0 else b[m].at[1 - y, :, c, :, cols]
                copies[i, RS1] = copy(i, RS1, src, r1.at[m, :, :, cols], nbr[axis])

    def rs2(i):
        m, lo, w, axis = slabs[i]
        cols = pl.ds(lo, w)
        copies[i, RS1].wait_recv()
        j = 1 - y if axis == 0 else 1 - x
        far = b[m].at[1 - y, x, c] if axis == 0 else b[m].at[y, 1 - x, c]
        add_to(far, r1.at[m, j], lo, w)
        copies[i, RS2] = copy(i, RS2, far.at[:, cols], r2.at[m, :, cols], nbr[1 - axis])
        add_to(b[m].at[y, x, c], r1.at[m, 1 - j], lo, w)

    def update(i):
        m, lo, w, axis = slabs[i]
        cs = slice(lo, lo + w)
        cols = pl.ds(lo, w)
        copies[i, RS2].wait_recv()
        own, out = b[m].at[y, x, c], g[m].at[y, x, c]

        def go(rows):
            mean = (own[rows, cs].astype(F32) + r2[m, rows, cs].astype(F32)) * rate
            state = hold_rate * sta[m, rows, cs] + mean
            new = par[m, rows, cs] - learn_rate * state
            out[rows, cs] = new.astype(BF16)
            sta[m, rows, cs] = state
            par[m, rows, cs] = new

        row_loop(chunk, step, go)
        copies[i, AG1] = copy(i, AG1, out.at[:, cols], out.at[:, cols], nbr[1 - axis])

    def ag2(i):
        m, lo, w, axis = slabs[i]
        cols = pl.ds(lo, w)
        copies[i, AG1].wait_recv()
        part = g[m].at[:, x, c, :, cols] if axis == 0 else g[m].at[y, :, c, :, cols]
        copies[i, AG2] = copy(i, AG2, part, part, nbr[axis])
        copies[i, SH1] = copy(i, SH1, part, part, mate)

    def share(i):
        m, lo, w, axis = slabs[i]
        cols = pl.ds(lo, w)
        copies[i, AG2].wait_recv()
        part = g[m].at[:, 1 - x, c, :, cols] if axis == 0 else g[m].at[1 - y, :, c, :, cols]
        copies[i, SH2] = copy(i, SH2, part, part, mate)

    def finish(i):
        m, lo, w, axis = slabs[i]
        cols = pl.ds(lo, w)
        copies[i, SH1].wait_recv()
        copies[i, SH2].wait_recv()
        if m == 1:
            for block in range(width // LANES):
                first, done, parts = block * LANES, 0, []
                while done < LANES:
                    k, off = divmod(first + done, chunk)
                    n = min(LANES - done, chunk - off)
                    parts.append(gd[k // 4, (k // 2) % 2, k % 2, off : off + n, lo : lo + w].astype(F32))
                    done += n
                whole = parts[0] if len(parts) == 1 else jnp.concatenate(parts, axis=0)
                hd[lo : lo + w, first : first + LANES] = whole.T.astype(BF16)

    pl.semaphore_wait(barrier, replicas - 1)
    vcopies = []
    for i in range(1, replicas):
        to = lax.rem(me + i, replicas)
        cp = pltpu.make_async_remote_copy(
            src_ref=vsend, dst_ref=vrecv.at[me],
            send_sem=vsend_sem.at[i], recv_sem=vrecv_sem.at[i],
            device_id={"dp": to}, device_id_type=pl.DeviceIdType.MESH,
        )
        cp.start()
        vcopies.append(cp)
    for i in range(0, count, 2):
        for j in (i, i + 1):
            convert(j)
            swap(j)
        for j in (i, i + 1):
            rs1(j)

    for cp in vcopies:
        cp.wait_recv()
    total = vrecv[0, :, 0:width]
    for k in range(1, replicas):
        total = total + vrecv[k, :, 0:width]
    lane = lax.broadcasted_iota(jnp.int32, (2, width), 1)

    def whole(at):
        full = jnp.zeros((2, width), F32)
        for k in range(replicas):
            piece = vrecv[k, :, at : at + vw]
            wide = jnp.concatenate([piece, jnp.zeros((2, width - vw), F32)], axis=1) if width > vw else piece
            moved = pltpu.roll(wide, k * chunk, 1) if k else wide
            full = jnp.where((lane >= k * chunk) & (lane < (k + 1) * chunk), moved, full)
        return full

    vstate = hold_rate * whole(width + vw) + total * rate
    vnext = whole(width) - learn_rate * vstate
    vhalf[...] = vnext
    for row, value in enumerate((vnext, vstate)):
        own = jnp.zeros((2, vw), F32)
        for k in range(replicas):
            moved = pltpu.roll(value, width - k * chunk, 1) if k else value
            own = jnp.where(me == k, moved[:, 0:vw], own)
        vown[row] = own

    for i in range(count):
        rs2(i)
    for cp in ploads:
        cp.wait()
    for i in range(count):
        update(i)
    order = list(range(per - 2)) + list(range(per, count)) + list(range(per - 2, per))
    for i in order:
        ag2(i)
    for n in range(0, count, 2):
        for i in order[n : n + 2]:
            share(i)
        for i in order[n : n + 2]:
            finish(i)
    for cp in copies.values():
        cp.wait_send()
    for cp in vcopies:
        cp.wait_send()


def columns_pad(n):
    return -(-n // LANES) * LANES


def write_out(gu, hd, par, sta, vown, vhalf, *refs):
    outs, (small, half_n, half_b, sem) = refs[:12], refs[12:]
    half = (half_n, half_b)
    chunk = small.shape[2]
    copies = []

    def move(src, dst):
        cp = pltpu.make_async_copy(src, dst, sem.at[len(copies)])
        cp.start()
        copies.append(cp)

    move(gu, outs[0])
    move(hd, outs[1])
    for i in range(4):
        small[i] = vown[i // 2, i % 2 : i % 2 + 1, 0:chunk]
    for i in range(2):
        half[i][...] = vhalf[i].astype(BF16)
    for i in range(4):
        move(small.at[i], outs[6 + i])
    for i in range(2):
        move(half[i], outs[10 + i])
    for i in range(4):
        move((par, sta)[i // 2].at[i % 2], outs[2 + i])
    for cp in copies:
        cp.wait()


def fused(slope_up, slope_down, slope_norm, slope_bias, param_up, param_down, param_norm, param_bias,
          state_up, state_down, state_norm, state_bias):
    replicas = lax.axis_size("dp")
    chunk, columns = param_up.shape
    width = replicas * chunk
    plan = slab_plan(columns)
    count = 2 * len(plan)
    vw = columns_pad(chunk)
    hbm = pl.BlockSpec(memory_space=pl.ANY)
    vmem = pl.BlockSpec(memory_space=pltpu.VMEM)
    main = pl.BlockSpec(memory_space=pltpu.MemorySpace.HBM)
    cube = (2, 2, 2, chunk, columns)
    shape = jax.ShapeDtypeStruct
    dma = pltpu.SemaphoreType.DMA
    far = lambda v: pltpu.with_memory_space_constraint(v, pltpu.MemorySpace.HBM)
    row = lambda v: far(v.reshape(1, -1))
    whole = width * columns
    scratch = 8 * whole + 6 * whole + (4 + 2 + 1) * 2 * whole // 8 * 2
    kept = pl.pallas_call(
        functools.partial(kernel, replicas, plan),
        out_shape=(
            pltpu.VMEM(cube, BF16), pltpu.VMEM((columns, width), BF16),
            pltpu.VMEM((2, chunk, columns), F32), pltpu.VMEM((2, chunk, columns), F32),
            pltpu.VMEM((2, 2, vw), F32), pltpu.VMEM((2, width), F32),
        ),
        in_specs=[main] * 12,
        out_specs=[vmem] * 6,
        scratch_shapes=[
            pltpu.VMEM((width, columns), F32), pltpu.VMEM((columns, width), F32),
            pltpu.VMEM(cube, BF16), pltpu.VMEM(cube, BF16),
            pltpu.VMEM((2, 2, 2, chunk, columns), BF16),
            pltpu.VMEM((2, 2, chunk, columns), BF16),
            pltpu.VMEM((2, chunk, columns), BF16),
            pltpu.VMEM(cube, BF16),
            pltpu.VMEM((2, width + 2 * vw), F32), pltpu.VMEM((replicas, 2, width + 2 * vw), F32),
            pltpu.VMEM((2, 1, width), F32), pltpu.VMEM((4, 1, chunk), F32),
            dma((7, count)), dma((7, count)), dma((replicas,)), dma((replicas,)),
            dma((count,)), dma((4,)), dma((6,)),
        ],
        compiler_params=pltpu.CompilerParams(
            collective_id=0, has_side_effects=True, vmem_limit_bytes=scratch + scratch // 8,
        ),
    )(
        far(slope_up), far(slope_down), far(slope_norm), far(slope_bias),
        far(param_up), far(param_down.T), row(param_norm), row(param_bias),
        far(state_up), far(state_down.T), row(state_norm), row(state_bias),
    )
    own = shape((1, chunk), F32)
    hu, hd, nu, nd, tu, td, nn, nb, tn, tb, hn, hb = pl.pallas_call(
        write_out,
        out_shape=(
            (shape(cube, BF16), shape((columns, width), BF16))
            + (shape((chunk, columns), F32),) * 4 + (own,) * 4 + (shape((width,), BF16),) * 2
        ),
        in_specs=[vmem] * 6,
        out_specs=[hbm] * 12,
        scratch_shapes=[
            pltpu.VMEM((4, 1, chunk), F32), pltpu.VMEM((width,), BF16), pltpu.VMEM((width,), BF16), dma((12,)),
        ],
        compiler_params=pltpu.CompilerParams(vmem_limit_bytes=4 * whole),
    )(*(pltpu.with_memory_space_constraint(v, pltpu.VMEM) for v in kept))
    return (
        hu.reshape(width, columns), hd, hn, hb,
        nu, nd.T, nn[0], nb[0],
        tu, td.T, tn[0], tb[0],
    )


def plain(slope_up, slope_down, slope_norm, slope_bias, param_up, param_down, param_norm, param_bias,
          state_up, state_down, state_norm, state_bias):
    rate = lax.axis_size("dp") ** (-0.5)
    place = lax.axis_index("dp")

    def step(mean, param, state):
        state_new = hold_rate * state + mean * rate
        return param - learn_rate * state_new, state_new

    def scattered(slope, dim):
        return lax.psum_scatter(slope[0].astype(BF16), "dp", scatter_dimension=dim, tiled=True).astype(F32)

    def gathered(value, dim):
        return lax.all_gather(value.astype(BF16), "dp", axis=dim, tiled=True)

    sums = lax.psum((slope_norm[0], slope_bias[0]), "dp")
    size = param_norm.shape[0]
    own = [lax.dynamic_slice_in_dim(v, place * size, size) for v in sums]
    nu, tu = step(scattered(slope_up, 0), param_up, state_up)
    nd, td = step(scattered(slope_down, 1), param_down, state_down)
    nn, tn = step(own[0], param_norm, state_norm)
    nb, tb = step(own[1], param_bias, state_bias)
    halves = gathered(nu, 0), gathered(nd, 1), gathered(nn, 0), gathered(nb, 0)
    return halves + (nu, nd, nn, nb, tu, td, tn, tb)


def body(*args):
    replicas = lax.axis_size("dp")
    chunk, columns = args[4].shape
    fits = replicas == 2 ** 3 and chunk % 16 == 0 and columns % (2 * LANES) == 0
    fits = fits and (replicas * chunk) % LANES == 0
    return (fused if fits else plain)(*args)


def solution(mesh):
    matrices = (P("dp", "tp"), P("tp", "dp"), P("dp"), P("dp"))
    return jax.shard_map(
        body,
        mesh=mesh,
        in_specs=(P("dp", None, "tp"), P("dp", "tp", None), P("dp", None), P("dp", None)) + matrices * 2,
        out_specs=(P(None, "tp"), P("tp", None), P(), P()) + matrices * 2,
        check_vma=False,
    )
```
